32 devices in a mesh: seq: 16 (over z, x, core), head: 2 (over y).
Axes of the slice: x: 2, y: 2, z: 4, core: 2. Of those that a mesh axis runs over, the one named last changes fastest.
Arguments:
- old_cache: bfloat16 [1024, 8, 128, 128], P(('seq', 'head')), may hold values from -9 to 9
- page_dest: int32 [1024], P(('seq', 'head')), may hold values from 0 to 1023, as said below
- seq_pages: int32 [32], replicated, may hold values from 1 to 64, 1024 in all
- last_fill: int32 [32], replicated, may hold values from 1 to 128
- queries: bfloat16 [32, 8, 512], P(None, 'head'), may hold values from -16 to 16
Outputs:
- new_cache: bfloat16 [1024, 8, 128, 128], P('seq', 'head')
- attended: bfloat16 [32, 8, 512], P('seq', 'head')
The draws below stay inside these ranges and needn't reach their ends.
Inputs may be any that keep to these rules, and one draw needn't show every extreme that they name: page_dest is a permutation of the page numbers. The 64 old pages p with the same p // 64 go to exactly 16 distinct new owners page_dest[p] // 64, exactly 4 pages to each; every new owner receives 64 pages.
All inputs are finite; a program needn't handle non-finite values.
Results may differ from the reference program's by a relative error of at most 0.004.
Values may be sent and summed in bfloat16 or wider, within the bound.
No kernel may reach another device: no remote copies, remote signals or barrier semaphores. Data moves between devices by JAX's collectives and lax.ppermute only.
A program may use at most 64 MiB of HBM per device.

```python
import math
import jax
import jax.numpy as jnp
import numpy as np
from jax import lax

KVH = 8
GROUP = 8
HD = 64
PAGE = 128
PAGES_DEV = 64
PAGES_ALL = 1024
SEQS = 32
MOST = 64
ROUTES = 16
CAP = 4
N_SEQ = 16
N_HEAD = 2


def draw_old_cache(key, part):
    key_first, key_second = jax.random.split(jax.random.fold_in(key, 11), 2)
    full_shape = (PAGES_ALL, KVH, PAGE, HD)
    key_part = jax.random.truncated_normal(key_first, -4.5, 4.5, full_shape, jnp.float32)
    value_part = jax.random.truncated_normal(key_second, -4.5, 4.5, full_shape, jnp.float32)
    return jnp.concatenate([key_part, value_part], axis=-1).astype(jnp.bfloat16)


def draw_queries(key, part):
    key_first = jax.random.fold_in(jax.random.fold_in(key, 23), 0)
    query_noise = 2.5 * jax.random.truncated_normal(key_first, -4.0, 4.0, (SEQS, KVH, GROUP, HD), jnp.float32)
    return query_noise.reshape(SEQS, KVH, GROUP * HD).astype(jnp.bfloat16)


def draw_page_dest(key, part):
    key_offsets, key_spans, key_pages, key_slots = jax.random.split(jax.random.fold_in(key, 37), 4)
    per_old = PAGES_DEV // N_HEAD
    offsets = jax.random.permutation(key_offsets, N_SEQ)[:ROUTES]
    span_order = jax.vmap(lambda subkey: jax.random.permutation(subkey, ROUTES))(jax.random.split(key_spans, N_SEQ))
    shuffles = jax.vmap(lambda subkey: jax.random.permutation(subkey, per_old))(jax.random.split(key_pages, N_SEQ * N_HEAD))
    slot_order = jax.vmap(lambda subkey: jax.random.permutation(subkey, PAGES_DEV))(jax.random.split(key_slots, N_SEQ))
    page_ids = jnp.arange(PAGES_ALL, dtype=jnp.int32)
    device_old = page_ids // per_old
    row_index = page_ids // PAGES_DEV
    within = page_ids % per_old
    position = shuffles[device_old, within]
    span_index = device_old % N_HEAD * (per_old // CAP) + position // CAP
    route_index = span_order[row_index, span_index]
    target = (row_index + offsets[route_index]) % N_SEQ
    slot_index = slot_order[target, route_index * CAP + position % CAP]
    return (target * PAGES_DEV + slot_index).astype(jnp.int32)


def with_ends(entries, own_key, smallest, high):
    longest = entries.shape.index(max(entries.shape))
    spots = []
    for shift in (0, 1):
        where = [jax.random.randint(jax.random.fold_in(own_key, axis), (), 0, length) for axis, length in enumerate(entries.shape)]
        where[longest] = (where[longest] + shift) % entries.shape[longest]
        spots.append(tuple(where))
    return entries.at[spots[0]].set(smallest).at[spots[1]].set(high)


def profile(number_of, total, limit, lean):
    loads = [(1 << 20) // math.isqrt(rank ** lean) + 1 for rank in range(2, number_of + 1)]
    surplus, counts = total - limit - (number_of - 1), [1] * (number_of - 1)
    while surplus > 0:
        free = [i for i in range(number_of - 1) if counts[i] < limit]
        whole, remaining = sum([loads[i] for i in free]), surplus
        for i in free:
            extra = min(limit - counts[i], max(1, remaining * loads[i] // whole), surplus)
            counts[i] = counts[i] + extra
            surplus = surplus - extra
    return np.array([limit] + counts)


def uneven(own_key, number_of, total, bound, slope):
    if number_of == 2:
        one = jax.random.randint(own_key, (), max(1, total - bound), min(bound, total - 1) + 1)
        return jnp.stack([one, total - one])
    sizes = jnp.asarray(profile(number_of, total, bound, slope), jnp.int32)
    twos = (number_of - 1) // 2
    giver, receiver = sizes[1:1 + 2 * twos:2], sizes[2:2 + 2 * twos:2]
    slack = jnp.minimum(giver - 1, bound - receiver)
    moved = jax.random.randint(jax.random.fold_in(own_key, 1), (twos,), 0, 1 << 20) % (slack + 1)
    sizes = sizes.at[1:1 + 2 * twos:2].set(giver - moved).at[2:2 + 2 * twos:2].set(receiver + moved)
    return sizes[jax.random.permutation(jax.random.fold_in(own_key, 2), number_of)]


def setup_inputs(seed: int = 0) -> dict:
    splits = jax.random.split(jax.random.key(seed), 6)
    return {
        "old_cache": draw_old_cache(jax.random.fold_in(splits[5], 71), 0),
        "page_dest": draw_page_dest(jax.random.fold_in(splits[5], 71), 0),
        "seq_pages": uneven(splits[2], SEQS, PAGES_ALL, MOST, 2).astype(jnp.int32),
        "last_fill": with_ends(jax.random.randint(splits[3], (SEQS,), 1, PAGE + 1), jax.random.fold_in(splits[3], 1), 1, PAGE).astype(jnp.int32),
        "queries": draw_queries(jax.random.fold_in(splits[5], 71), 0),
    }


NEG_FILL = -1.0e30


def reference(old_cache, page_dest, seq_pages, last_fill, queries):
    new_cache = jnp.zeros_like(old_cache).at[page_dest].set(old_cache)
    page_ids = jnp.arange(PAGES_ALL, dtype=jnp.int32)
    position = ((page_ids % PAGES_DEV) * N_SEQ + page_ids // PAGES_DEV).astype(jnp.int32)
    seq_ends = jnp.cumsum(seq_pages).astype(jnp.int32)
    page_owner = jnp.sum((position[:, None] >= seq_ends[None, :]).astype(jnp.int32), axis=1).astype(jnp.int32)
    member = page_owner[None, :] == jnp.arange(SEQS, dtype=jnp.int32)[:, None]
    owner_end = jnp.take(seq_ends, page_owner)
    owner_fill = jnp.take(last_fill, page_owner)
    page_fill = jnp.where(position == owner_end - 1, owner_fill, PAGE)
    token_live = jnp.arange(PAGE, dtype=jnp.int32)[None, :] < page_fill[:, None]
    scale_factor = HD ** -0.5
    member_float = member.astype(jnp.float32)

    def one_head(operands):
        head_cache, head_query = operands
        page_query = jnp.take(head_query, page_owner, axis=0).astype(jnp.float32).reshape(PAGES_ALL, GROUP, HD)
        key_part = head_cache[:, :, :HD].astype(jnp.float32)
        value_part = head_cache[:, :, HD:].astype(jnp.float32)
        scores = jnp.einsum("pgd,ptd->pgt", page_query, key_part, precision=lax.Precision.HIGHEST) * scale_factor
        scores = jnp.where(token_live[:, None, :], scores, NEG_FILL)
        page_max = jnp.max(scores, axis=2)
        seq_max = jnp.max(jnp.where(member[:, :, None], page_max[None, :, :], NEG_FILL), axis=1)
        owner_max = jnp.take(seq_max, page_owner, axis=0)
        weights = jnp.where(token_live[:, None, :], jnp.exp(scores - owner_max[:, :, None]), 0.0).astype(jnp.bfloat16)
        weights = lax.optimization_barrier(weights).astype(jnp.float32)
        page_total = jnp.sum(weights, axis=2)
        page_sum = jnp.einsum("pgt,ptd->pgd", weights, value_part, precision=lax.Precision.HIGHEST)
        totals = jnp.dot(member_float, page_total, precision=lax.Precision.HIGHEST)
        weighted = jnp.dot(member_float, page_sum.reshape(PAGES_ALL, GROUP * HD), precision=lax.Precision.HIGHEST)
        result = weighted.reshape(SEQS, GROUP, HD) / totals[:, :, None]
        return result.reshape(SEQS, GROUP * HD)

    head_first = jnp.moveaxis(new_cache, 1, 0)
    attended = lax.map(one_head, (head_first, jnp.moveaxis(queries, 1, 0)))
    attended = jnp.moveaxis(attended, 0, 1).astype(jnp.bfloat16)
    return new_cache, attended
```

```python
import functools
import jax
import jax.numpy as jnp
from jax import lax
from jax.experimental import pallas as pl
from jax.experimental.pallas import tpu as pltpu
from jax.sharding import PartitionSpec as P

NEG_FILL = -1e30
LABEL_ROWS = 8

ANY = pl.BlockSpec(memory_space=pl.ANY)
SMEM = pl.BlockSpec(memory_space=pltpu.SMEM)
VMEM = pl.BlockSpec(memory_space=pltpu.VMEM)


def chunk_rows(rows):
    eighths = (1, 3, 4)
    unit = rows // 8
    edges, start = [], 0
    for share in eighths:
        edges.append((start, share * unit))
        start += share * unit
    return edges


def pack_kernel(sizes, *refs):
    pages_own, page_count, peers, cap, rows, start, length, groups, extra, label = sizes
    dest, head_id, old = refs[:3]
    received = refs[3:3 + groups - 1]
    refs = refs[3 + groups - 1:]
    tail = None
    if extra and not label:
        tail, refs = refs[0], refs[1:]
    out, stage, counts, places, slots, label_tile, in_sem, out_sem, tail_sem = refs
    offset = pl.multiple_of(head_id[0] * rows + start, 8)
    copies = [pltpu.make_async_copy(
        old.at[:, pl.ds(offset, length), :], stage.at[pl.ds(0, pages_own)], in_sem.at[0])]
    for j, block in enumerate(received):
        copies.append(pltpu.make_async_copy(
            block, stage.at[pl.ds((j + 1) * pages_own, pages_own)], in_sem.at[j + 1]))
    for copy in copies:
        copy.start()
    if tail is not None:
        tail_copy = pltpu.make_async_copy(
            tail, out.at[:, pl.ds(cap * length, extra), :], tail_sem)
        tail_copy.start()

    @pl.loop(0, peers)
    def _(t):
        counts[t] = 0

    if label:
        @pl.loop(0, peers * cap)
        def _(i):
            slots[i] = -1

    @pl.loop(0, page_count)
    def _(p):
        d = dest[p]
        t = d // page_count
        n = counts[t]
        counts[t] = n + 1
        places[p] = t * cap + n
        if label:
            slots[t * cap + n] = d - t * page_count

    def page_copy(p):
        place = places[p]
        t = place // cap
        row = pl.multiple_of((place - t * cap) * length, 8)
        return pltpu.make_async_copy(
            stage.at[p], out.at[t, pl.ds(row, length), :], out_sem.at[p])

    if label:
        lane = lax.broadcasted_iota(jnp.int32, (extra, 128), 1)

        @pl.loop(0, peers)
        def _(t):
            tile = jnp.full((extra, 128), -1, jnp.int32)
            for n in range(cap):
                tile = jnp.where(lane == n, slots[t * cap + n], tile)
            label_tile[t] = tile.astype(jnp.float32).astype(jnp.bfloat16)

        tail_copy = pltpu.make_async_copy(
            label_tile, out.at[:, pl.ds(cap * length, extra), :], tail_sem)
        tail_copy.start()
    for j in range(groups):
        copies[j].wait()

        @pl.loop(j * pages_own, (j + 1) * pages_own)
        def _(p):
            page_copy(p).start()

    @pl.loop(0, page_count)
    def _(p):
        page_copy(p).wait()

    if extra:
        tail_copy.wait()


def pack(dest, head_id, old, received, tail, geometry, start, length, label):
    pages_own, page_count, peers, cap, rows, groups = geometry
    extra = LABEL_ROWS if label else (tail.shape[1] if tail is not None else 0)
    sizes = (pages_own, page_count, peers, cap, rows, start, length, groups, extra, label)
    operands = [dest, head_id, old, *received] + ([tail] if tail is not None else [])
    specs = [SMEM, SMEM] + [ANY] * groups + ([VMEM] if tail is not None else [])
    moved = 4 * page_count * length * 128
    return pl.pallas_call(
        functools.partial(pack_kernel, sizes),
        out_shape=jax.ShapeDtypeStruct((peers, cap * length + extra, 128), jnp.bfloat16),
        in_specs=specs,
        out_specs=ANY,
        scratch_shapes=[
            pltpu.VMEM((page_count, length, 128), jnp.bfloat16),
            pltpu.SMEM((peers,), jnp.int32),
            pltpu.SMEM((page_count,), jnp.int32),
            pltpu.SMEM((peers * cap,), jnp.int32),
            pltpu.VMEM((peers, LABEL_ROWS, 128), jnp.bfloat16),
            pltpu.SemaphoreType.DMA((groups,)),
            pltpu.SemaphoreType.DMA((page_count,)),
            pltpu.SemaphoreType.DMA,
        ],
        cost_estimate=pl.CostEstimate(flops=moved * 4, bytes_accessed=moved, transcendentals=0),
        name="pack",
    )(*operands)


def merge_partials(tail, attended, peers, local, width, rows):
    lane = lax.broadcasted_iota(jnp.int32, (rows, 128), 1)
    row = lax.broadcasted_iota(jnp.int32, (rows, 128), 0)
    diagonal = lane == row
    parts = local * rows
    for s in range(local):
        logs = []
        top = jnp.full((rows, 1), NEG_FILL, jnp.float32)
        for t in range(peers):
            scale_rows = tail[t, parts:parts + 8, :].astype(jnp.float32)
            line = jnp.sum(scale_rows[3 * s:3 * s + 3], axis=0, keepdims=True)
            line = jnp.where(diagonal, jnp.broadcast_to(line, (rows, 128)), 0.0)
            value = jnp.sum(line, axis=1, keepdims=True)
            logs.append(value)
            top = jnp.maximum(top, value)
        total = jnp.zeros((rows, 1), jnp.float32)
        summed = jnp.zeros((rows, 128), jnp.float32)
        for t in range(peers):
            scale = jnp.exp(logs[t] - top)
            total = total + scale
            summed = summed + scale * tail[t, s * rows:(s + 1) * rows, :].astype(jnp.float32)
        values = summed[:, width:] + summed[:, :width]
        attended[s] = (values / total).astype(jnp.bfloat16)


def place_kernel(sizes, *refs):
    _, peers, cap, start, length, extra, first, local, width, rows = sizes
    labels, incoming = refs[:2]
    refs = refs[2:] if first else refs[3:]
    cache = refs[0]
    refs = refs[1:]
    if extra:
        attended, refs = refs[0], refs[1:]
    stage, in_sem, out_sem = refs[:3]
    if extra:
        tail, tail_sem = refs[3:]
        tail_copy = pltpu.make_async_copy(
            incoming.at[:, pl.ds(cap * length, extra), :], tail, tail_sem)
        tail_copy.start()

    def block_copy(t):
        return pltpu.make_async_copy(
            incoming.at[t, pl.ds(0, cap * length), :], stage.at[t], in_sem.at[t])

    def page_copy(t, n):
        i = t * cap + n
        return pltpu.make_async_copy(
            stage.at[t, pl.ds(n * length, length), :],
            cache.at[labels[i], pl.ds(start, length), :], out_sem.at[i])

    @pl.loop(0, peers)
    def _(t):
        block_copy(t).start()

    @pl.loop(0, peers)
    def _(t):
        block_copy(t).wait()
        for n in range(cap):
            @pl.when(labels[t * cap + n] >= 0)
            def _():
                page_copy(t, n).start()

    if extra:
        tail_copy.wait()
        merge_partials(tail, attended, peers, local, width, rows)

    @pl.loop(0, peers)
    def _(t):
        for n in range(cap):
            @pl.when(labels[t * cap + n] >= 0)
            def _():
                page_copy(t, n).wait()


def place(labels, incoming, cache, geometry, start, length, merged):
    _, page_count, peers, cap, rows, _ = geometry
    local, kj, width = merged if merged else (0, 0, 0)
    extra = incoming.shape[1] - cap * length if merged else 0
    first = cache is None
    sizes = (page_count, peers, cap, start, length, extra, first, local, width, kj)
    operands = [labels, incoming] + ([] if first else [cache])
    outs = [jax.ShapeDtypeStruct((page_count, rows, 128), jnp.bfloat16)]
    out_specs = [ANY]
    scratch = [
        pltpu.VMEM((peers, cap * length, 128), jnp.bfloat16),
        pltpu.SemaphoreType.DMA((peers,)),
        pltpu.SemaphoreType.DMA((peers * cap,)),
    ]
    if extra:
        outs.append(jax.ShapeDtypeStruct((local, kj, width), jnp.bfloat16))
        out_specs.append(VMEM)
        scratch += [pltpu.VMEM((peers, extra, 128), jnp.bfloat16), pltpu.SemaphoreType.DMA]
    moved = 4 * page_count * length * 128
    return pl.pallas_call(
        functools.partial(place_kernel, sizes),
        out_shape=outs,
        in_specs=[SMEM, ANY] + ([] if first else [ANY]),
        out_specs=out_specs,
        scratch_shapes=scratch,
        input_output_aliases={} if first else {2: 0},
        cost_estimate=pl.CostEstimate(flops=moved * 4, bytes_accessed=moved, transcendentals=0),
        name="place",
    )(*operands)


def attend_kernel(sizes, *refs):
    pages_own, page_count, peers, rows, groups, chunks, kj, width, page_len, local = sizes
    owner, fill, head_id, query, old = refs[:5]
    blocks = refs[5:5 + len(chunks) * (groups - 1)]
    (out, stage, tile_max, tile_total, tile_sum,
     seq_max, seq_total, seq_sum, sems) = refs[5 + len(blocks):]
    heads = rows // page_len
    group = kj // heads
    offset = pl.multiple_of(head_id[0] * rows, 8)
    copies = [pltpu.make_async_copy(
        old.at[:, pl.ds(offset, rows), :], stage.at[pl.ds(0, pages_own)], sems.at[0])]
    for j in range(groups - 1):
        for c, (start, length) in enumerate(chunks):
            i = j * len(chunks) + c
            copies.append(pltpu.make_async_copy(
                blocks[i],
                stage.at[pl.ds((j + 1) * pages_own, pages_own), pl.ds(start, length), :],
                sems.at[i + 1]))
    for copy in copies:
        copy.start()
    seq_max[...] = jnp.full_like(seq_max, NEG_FILL)
    seq_total[...] = jnp.zeros_like(seq_total)
    seq_sum[...] = jnp.zeros_like(seq_sum)
    for copy in copies:
        copy.wait()
    token = lax.broadcasted_iota(jnp.int32, (group, page_len), 1)
    scale = width ** -0.5

    @pl.loop(0, page_count, unroll=2)
    def _(p):
        s = owner[p]
        live = token < fill[p]
        for k in range(heads):
            page = stage[p, k * page_len:(k + 1) * page_len, :]
            q = query[s, k * group:(k + 1) * group, :]
            scores = lax.dot_general(
                q, page, (((1,), (1,)), ((), ())), preferred_element_type=jnp.float32) * scale
            scores = jnp.where(live, scores, NEG_FILL)
            top = jnp.max(scores, axis=1, keepdims=True)
            weights = jnp.where(live, jnp.exp(scores - top), 0.0).astype(jnp.bfloat16)
            total = jnp.sum(weights.astype(jnp.float32), axis=1, keepdims=True)
            here = pl.ds(k * group, group)
            tile_sum[p, here, :] = jnp.dot(weights, page, preferred_element_type=jnp.float32)
            tile_max[p, here, :] = jnp.broadcast_to(top, (group, 128))
            tile_total[p, here, :] = jnp.broadcast_to(total, (group, 128))

    @pl.loop(0, page_count)
    def _(p):
        s = owner[p]
        seq_max[s] = jnp.maximum(seq_max[s], tile_max[p])

    @pl.loop(0, page_count)
    def _(p):
        s = owner[p]
        factor = jnp.exp(tile_max[p] - seq_max[s])
        seq_total[s] = seq_total[s] + factor * tile_total[p]
        seq_sum[s] = seq_sum[s] + factor * tile_sum[p]

    lane = lax.broadcasted_iota(jnp.int32, (kj, 128), 1)
    diagonal = lane == lax.broadcasted_iota(jnp.int32, (kj, 128), 0)
    parts = local * kj

    @pl.loop(0, peers)
    def _(t):
        lines = []
        for i in range(local):
            s = t * local + i
            total = seq_total[s]
            some = total > 0.0
            safe = jnp.where(some, total, 1.0)
            value = jnp.where(some, seq_sum[s] / safe, 0.0)
            high = value.astype(jnp.bfloat16).astype(jnp.float32)
            low = pltpu.roll(value - high, 128 - width, 1)
            out[t, i * kj:(i + 1) * kj, :] = jnp.where(lane < width, low, high).astype(jnp.bfloat16)
            log = jnp.where(some, seq_max[s] + jnp.log(safe), NEG_FILL)
            for _ in range(3):
                part = log.astype(jnp.bfloat16).astype(jnp.float32)
                log = log - part
                lines.append(jnp.sum(jnp.where(diagonal, part, 0.0), axis=0, keepdims=True))
        while len(lines) % 8:
            lines.append(jnp.zeros((1, 128), jnp.float32))
        out[t, parts:parts + len(lines), :] = jnp.concatenate(lines, 0).astype(jnp.bfloat16)


def attend(owner, fill, head_id, query, old, received, geometry, chunks, width, page_len):
    pages_own, page_count, peers, _, rows, groups = geometry
    seqs, kj, _ = query.shape
    local = seqs // peers
    extra = local * kj + (3 * local + 7) // 8 * 8
    blocks = [received[c][j] for j in range(groups - 1) for c in range(len(chunks))]
    sizes = (pages_own, page_count, peers, rows, groups, chunks, kj, width, page_len, local)
    return pl.pallas_call(
        functools.partial(attend_kernel, sizes),
        out_shape=jax.ShapeDtypeStruct((peers, extra, 128), jnp.bfloat16),
        in_specs=[SMEM, SMEM, SMEM, VMEM, ANY] + [ANY] * len(blocks),
        out_specs=VMEM,
        scratch_shapes=[
            pltpu.VMEM((page_count, rows, 128), jnp.bfloat16),
            pltpu.VMEM((page_count, kj, 128), jnp.float32),
            pltpu.VMEM((page_count, kj, 128), jnp.float32),
            pltpu.VMEM((page_count, kj, 128), jnp.float32),
            pltpu.VMEM((seqs, kj, 128), jnp.float32),
            pltpu.VMEM((seqs, kj, 128), jnp.float32),
            pltpu.VMEM((seqs, kj, 128), jnp.float32),
            pltpu.SemaphoreType.DMA((len(blocks) + 1,)),
        ],
        cost_estimate=pl.CostEstimate(
            flops=page_count * kj * page_len * 512 * 16, bytes_accessed=2 * page_count * rows * 128,
            transcendentals=page_count * kj * page_len),
        name="attend",
    )(owner, fill, head_id, query, old, *blocks)


def page_layout(dest, seq_pages, last_fill, page_len, page_count, peers):
    position = dest % page_count * peers + dest // page_count
    seqs = seq_pages.shape[0]
    ids = jnp.arange(seqs, dtype=jnp.int32)
    ends = jnp.sum(jnp.where(ids[:, None] <= ids[None, :], seq_pages[:, None], 0), axis=0)
    owner = jnp.sum((position[:, None] >= ends[None, :]).astype(jnp.int32), axis=1)
    member = owner[:, None] == ids[None, :]
    last = jnp.any(member & (position[:, None] == ends[None, :] - 1), axis=1)
    owner_fill = jnp.sum(jnp.where(member, last_fill[None, :], 0), axis=1)
    return owner, jnp.where(last, owner_fill, page_len)


def per_device(old_cache, page_dest, seq_pages, last_fill, queries):
    pages_own, all_heads, page_len, double = old_cache.shape
    groups = lax.axis_size("head")
    peers = lax.axis_size("seq")
    head = lax.axis_index("head").astype(jnp.int32)
    width = double // 2
    heads = all_heads // groups
    rows = heads * page_len
    page_count = pages_own * groups
    cap = page_count // min(peers, 16)
    seqs = queries.shape[0]
    kj = heads * (queries.shape[2] // width)
    geometry = (pages_own, page_count, peers, cap, rows, groups)
    chunks = tuple(chunk_rows(rows))
    old = old_cache.reshape(pages_own, all_heads * page_len, double)
    head_id = head[None]

    def shift(x, j):
        return lax.ppermute(x, "head", [(i, (i + j) % groups) for i in range(groups)])

    received, source = [], old
    dests = [page_dest]
    for c, (start, length) in enumerate(chunks):
        pieces = []
        for j in range(1, groups):
            target = (head + j) % groups
            pieces.append(lax.dynamic_slice(
                source, (0, target * rows + start, 0), (pages_own, length, double)))
        source, pieces = lax.optimization_barrier((source, pieces))
        received.append([shift(piece, j) for j, piece in enumerate(pieces, 1)])
        if c == 0:
            dests += [shift(page_dest, j) for j in range(1, groups)]
    dest = jnp.concatenate(dests)
    query = jnp.pad(queries.reshape(seqs, kj, width), ((0, 0), (0, 0), (0, double - width)))
    owner, fill = page_layout(dest, seq_pages, last_fill, page_len, page_count, peers)
    cache = labels = None
    for c, (start, length) in enumerate(chunks):
        final = c == len(chunks) - 1
        tail = None
        if final:
            tail = attend(owner, fill, head_id, query, old, received, geometry, chunks,
                          width, page_len)
        outgoing = pack(dest, head_id, old, received[c], tail, geometry, start, length, c == 0)
        incoming = lax.all_to_all(outgoing, "seq", split_axis=0, concat_axis=0, tiled=True)
        if c == 0:
            labels = incoming[:, cap * length, :cap].astype(jnp.int32).reshape(-1)
        merged = (seqs // peers, kj, width) if final else None
        outs = place(labels, incoming, cache, geometry, start, length, merged)
        cache = outs[0]
    attended = outs[1].reshape(seqs // peers, heads, -1)
    return cache.reshape(page_count, heads, page_len, double), attended


def solution(mesh):
    in_specs = (
        P(("seq", "head"), None, None, None),
        P(("seq", "head")),
        P(),
        P(),
        P(None, "head", None),
    )
    out_specs = (P("seq", "head", None, None), P("seq", "head", None))
    return jax.shard_map(
        per_device, mesh=mesh, in_specs=in_specs, out_specs=out_specs, check_vma=False
    )
```

```python
import functools
import jax
import jax.numpy as jnp
from jax import lax
from jax.experimental import pallas as pl
from jax.experimental.pallas import tpu as pltpu
from jax.sharding import PartitionSpec as P

NEG_FILL = -1e30
LABEL_ROWS = 8
SHARES = (1, 2, 3, 4, 8, 8, 6)
KINDS = ("fwd", "fwd", "fwd", "fwd", "all", "far", "all")

HBM = pl.BlockSpec(memory_space=pltpu.HBM)
SMEM = pl.BlockSpec(memory_space=pltpu.SMEM)
VMEM = pl.BlockSpec(memory_space=pltpu.VMEM)


def partner(me, k, peers):
    if peers & (peers - 1) == 0:
        return me ^ k
    return (me + k) % peers


def sender(me, k, peers):
    if peers & (peers - 1) == 0:
        return me ^ k
    return (me + peers - k) % peers


class Geometry:
    def __init__(self, pages_own, groups, peers, rows):
        self.pages_own, self.groups, self.peers, self.rows = pages_own, groups, peers, rows
        self.page_count = pages_own * groups
        self.cap = self.page_count // min(peers, 16)
        self.full = peers * self.cap == self.page_count


def spread(pieces):
    offset, laid = 0, []
    for start, length in pieces:
        laid.append((start, length, offset))
        offset += length
    return laid, offset


def granted(*sizes):
    return pltpu.CompilerParams(vmem_limit_bytes=(4 << 20) + sum(sizes))


def estimate(moved):
    return pl.CostEstimate(flops=moved * 4, bytes_accessed=moved, transcendentals=0)


def pack_kernel(g, ks, single, pieces, passed, extra, label, *refs):
    laid, length = spread(pieces)
    dests, old, refs = refs[:g.groups], refs[g.groups], refs[g.groups + 1:]
    count = len(pieces) * (g.groups - 1)
    received, refs = refs[:count], refs[count:]
    head, me = lax.axis_index("head"), lax.axis_index("seq")
    forwarded, refs = refs[:len(passed)], refs[len(passed):]
    tail = None
    if extra and not label:
        tail, refs = refs[0], refs[1:]
    number = g.peers if ks is None else len(ks)
    if single:
        outs, refs = [refs[0].at[i] for i in range(number)], refs[1:]
    else:
        outs, refs = refs[:number], refs[number:]
    if ks is None:
        targets = list(range(g.peers))
    else:
        targets = [partner(me, k, g.peers) for k in ks]
    stage, counts, order, slot, in_sem, out_sem = refs[:6]
    pass_stages, refs = refs[6:6 + len(passed)], refs[6 + len(passed):]
    copies = []
    for c, (start, size, offset) in enumerate(laid):
        row = pl.multiple_of(head * g.rows + start, 8)
        copies.append(pltpu.make_async_copy(
            old.at[:, pl.ds(row, size), :],
            stage.at[pl.ds(0, g.pages_own), pl.ds(offset, size), :], in_sem.at[c]))
        for j in range(1, g.groups):
            i = (j - 1) * len(pieces) + c
            copies.append(pltpu.make_async_copy(
                received[i],
                stage.at[pl.ds(j * g.pages_own, g.pages_own), pl.ds(offset, size), :],
                in_sem.at[len(pieces) + i]))
    arrivals = []
    if passed:
        pass_in, pass_out = refs
        arrivals = [pltpu.make_async_copy(block, place, pass_in.at[c]) for c, (block, place)
                    in enumerate(zip(forwarded, pass_stages))]
    for copy in copies + arrivals:
        copy.start()

    @pl.loop(0, g.peers, unroll=8)
    def _(t):
        counts[t] = 0

    if not g.full:
        @pl.loop(0, g.peers * g.cap)
        def _(i):
            order[i] = -1

    for j, dest in enumerate(dests):
        @pl.loop(0, g.pages_own, unroll=8)
        def _(i):
            d = dest[i]
            if g.page_count & (g.page_count - 1) == 0:
                t = lax.shift_right_logical(d, g.page_count.bit_length() - 1)
            else:
                t = d // g.page_count
            n = counts[t]
            counts[t] = n + 1
            order[t * g.cap + n] = j * g.pages_own + i
            if label:
                slot[t * g.cap + n] = d - t * g.page_count

    for i, t in enumerate(targets):
        block = outs[i]
        if tail is not None:
            block[g.cap * length:, :] = tail[t]
        if label:
            lane = lax.broadcasted_iota(jnp.int32, (extra, 128), 1)
            tile = jnp.full((extra, 128), -1, jnp.int32)
            for n in range(g.cap):
                value = slot[t * g.cap + n]
                if not g.full:
                    value = jnp.where(order[t * g.cap + n] >= 0, value, -1)
                tile = jnp.where(lane == n, value, tile)
            block[g.cap * length:, :] = tile.astype(jnp.float32).astype(jnp.bfloat16)
    for copy in copies:
        copy.wait()
    if not passed:
        for i, t in enumerate(targets):
            for n in range(g.cap):
                p = order[t * g.cap + n]
                outs[i][n * length:(n + 1) * length, :] = stage[p if g.full else jnp.maximum(p, 0)]
        return

    def page_copy(i, n, p):
        return pltpu.make_async_copy(
            stage.at[p], outs[i].at[pl.ds(n * length, length), :], out_sem.at[i])

    for step in ("start",) if g.full else ("start", "wait"):
        for i, t in enumerate(targets):
            for n in range(g.cap):
                p = order[t * g.cap + n]
                if g.full:
                    page_copy(i, n, p).start()
                else:
                    @pl.when(p >= 0)
                    def _():
                        getattr(page_copy(i, n, p), step)()
    base, passes = g.cap * length, []
    for c, size in enumerate(passed):
        arrivals[c].wait()
        for i in range(number):
            passes.append(pltpu.make_async_copy(
                pass_stages[c].at[i], outs[i].at[pl.ds(base, g.cap * size), :], pass_out.at[c, i]))
            passes[-1].start()
        base += g.cap * size
    if g.full:
        for i in range(len(targets)):
            block = outs[i].at[pl.ds(0, g.cap * length), :]
            pltpu.make_async_copy(block, block, out_sem.at[i]).wait()
    for copy in passes:
        copy.wait()


def pack(g, ks, dests, old, pieces, received, tail=None, label=False, single=True,
         passed=(), forwarded=()):
    _, length = spread(pieces)
    extra = LABEL_ROWS if label else (tail.shape[1] if tail is not None else 0)
    blocks = [received[c][j] for j in range(g.groups - 1) for c in range(len(pieces))]
    operands = [*dests, old, *blocks, *forwarded] + ([tail] if tail is not None else [])
    shape = (g.cap * (length + sum(passed)) + extra, 128)
    number = g.peers if ks is None else len(ks)
    if single:
        outs = [jax.ShapeDtypeStruct((number,) + shape, jnp.bfloat16)]
    else:
        outs = [jax.ShapeDtypeStruct(shape, jnp.bfloat16)] * number
    scratch = [
        pltpu.VMEM((g.page_count, length, 128), jnp.bfloat16),
        pltpu.SMEM((g.peers,), jnp.int32),
        pltpu.SMEM((g.peers * g.cap,), jnp.int32),
        pltpu.SMEM((g.peers * g.cap,), jnp.int32),
        pltpu.SemaphoreType.DMA((len(pieces) * g.groups,)),
        pltpu.SemaphoreType.DMA((number,)),
    ]
    scratch += [pltpu.VMEM((number, g.cap * size, 128), jnp.bfloat16) for size in passed]
    if passed:
        scratch += [pltpu.SemaphoreType.DMA((len(passed),)),
                    pltpu.SemaphoreType.DMA((len(passed), number))]
    return pl.pallas_call(
        functools.partial(pack_kernel, g, ks, single, pieces, passed, extra, label),
        out_shape=outs,
        in_specs=[SMEM] * g.groups + [HBM] * (1 + len(blocks) + len(forwarded))
        + ([VMEM] if tail is not None else []),
        out_specs=[HBM if passed else VMEM] * len(outs),
        scratch_shapes=scratch,
        cost_estimate=estimate(4 * number * g.cap * length * 128),
        name="pack",
    )(*operands)


def labels_kernel(g, row, blocks, out, raw, lines, sem, out_sem):
    copy = pltpu.make_async_copy(blocks.at[:, pl.ds(row, LABEL_ROWS), :], raw, sem)
    copy.start()
    copy.wait()
    for i in range(g.peers):
        lines[i:i + 1, :] = raw[i].astype(jnp.float32)[:1].astype(jnp.int32)
    move = pltpu.make_async_copy(lines, out, out_sem)
    move.start()
    move.wait()


def read_labels(g, blocks, row):
    return pl.pallas_call(
        functools.partial(labels_kernel, g, row),
        out_shape=jax.ShapeDtypeStruct((g.peers, 128), jnp.int32),
        in_specs=[HBM],
        out_specs=SMEM,
        scratch_shapes=[
            pltpu.VMEM((g.peers, LABEL_ROWS, 128), jnp.bfloat16),
            pltpu.VMEM((g.peers, 128), jnp.int32),
            pltpu.SemaphoreType.DMA,
            pltpu.SemaphoreType.DMA,
        ],
        compiler_params=granted(),
        cost_estimate=estimate(g.peers * 4096),
        name="labels",
    )(blocks)


def merge_partials(tails, attended, local, width, rows):
    lane = lax.broadcasted_iota(jnp.int32, (rows, 128), 1)
    diagonal = lane == lax.broadcasted_iota(jnp.int32, (rows, 128), 0)
    shared = 128 // width
    parts = (local + shared - 1) // shared * rows
    lines = [tail[parts:, :].astype(jnp.float32) for tail in tails]
    weights = []
    for s in range(local):
        logs = [jnp.sum(line[3 * s:3 * s + 3], axis=0, keepdims=True) for line in lines]
        top = functools.reduce(jnp.maximum, logs)
        scales = [jnp.exp(log - top) for log in logs]
        total = sum(scales)
        weights.append([scale / total for scale in scales])
    group = attended.shape[2] // width
    for first in range(0, local, shared):
        summed = jnp.zeros((rows, 128), jnp.float32)
        held = range(first, min(first + shared, local))
        for t, tail in enumerate(tails):
            scale = jnp.zeros((rows, 128), jnp.float32)
            for s in held:
                line = jnp.where(diagonal, jnp.broadcast_to(weights[s][t], (rows, 128)), 0.0)
                column = jnp.broadcast_to(jnp.sum(line, axis=1, keepdims=True), (rows, 128))
                scale = jnp.where(lane < 128 - width * (s - first), column, scale)
            row = first // shared * rows
            summed = summed + scale * tail[row:row + rows, :].astype(jnp.float32)
        for s in held:
            end = 128 - width * (s - first)
            values = summed[:, end - width:end].astype(jnp.bfloat16)
            for row in range(rows):
                k, j = row // group, row % group
                attended[s, k:k + 1, j * width:(j + 1) * width] = values[row:row + 1]


def place_kernel(g, ks, pieces, passed, first, merged, tail_rows, *refs):
    laid, length = spread(pieces)
    labels, refs = refs[0], refs[1:]
    me = lax.axis_index("seq")
    if ks is None:
        blocks, refs = [refs[0].at[t] for t in range(g.peers)], refs[1:]
        indices = list(range(g.peers))
    else:
        blocks, refs = refs[:len(ks)], refs[len(ks):]
        indices = [sender(me, k, g.peers) for k in ks]
    refs = refs if first else refs[1:]
    cache, refs = refs[0], refs[1:]
    if merged:
        attended, refs = refs[0], refs[1:]
    out_sem = refs[0]

    def each_page(act):
        for i, (block, index) in enumerate(zip(blocks, indices)):
            for n in range(g.cap):
                label = labels[index, n]

                def run():
                    for start, size, offset in laid:
                        getattr(pltpu.make_async_copy(
                            block.at[pl.ds(n * length + offset, size), :],
                            cache.at[label, pl.ds(start, size), :], out_sem.at[i]), act)()

                if g.full:
                    run()
                else:
                    pl.when(label >= 0)(run)
                if not passed:
                    continue
                other = labels[sender(index, g.peers // 2, g.peers), n]

                def run_passed():
                    base = g.cap * length
                    for start, size in passed:
                        getattr(pltpu.make_async_copy(
                            block.at[pl.ds(base + n * size, size), :],
                            cache.at[other, pl.ds(start, size), :], out_sem.at[i]), act)()
                        base += g.cap * size

                if g.full:
                    run_passed()
                else:
                    pl.when(other >= 0)(run_passed)

    each_page("start")
    if merged:
        merge_partials([block.at[pl.ds(g.cap * length, tail_rows), :] for block in blocks],
                       attended, *merged)
    if g.full:
        for i, block in enumerate(blocks):
            rows = g.cap * (length + sum(size for _, size in passed))
            moved = block.at[pl.ds(0, rows), :]
            pltpu.make_async_copy(moved, moved, out_sem.at[i]).wait()
    else:
        each_page("wait")


def place(g, ks, labels, blocks, cache, pieces, passed=(), merged=None, shape=None):
    first = cache is None
    _, length = spread(pieces)
    operands = [labels, *blocks] + ([] if first else [cache])
    outs = [jax.ShapeDtypeStruct((g.page_count, g.rows, 128), jnp.bfloat16)]
    out_specs = [HBM]
    if merged:
        outs.append(jax.ShapeDtypeStruct(shape, jnp.bfloat16))
        out_specs.append(VMEM)
    number = g.peers if ks is None else len(ks)
    return pl.pallas_call(
        functools.partial(place_kernel, g, ks, pieces, passed, first, merged,
                          blocks[0].shape[-2] - g.cap * length),
        out_shape=outs,
        in_specs=[SMEM] + [VMEM] * len(blocks) + [HBM] * (0 if first else 1),
        out_specs=out_specs,
        scratch_shapes=[pltpu.SemaphoreType.DMA((number,))],
        compiler_params=granted(2 * number * blocks[0].shape[-2] * 128),
        input_output_aliases={} if first else {len(operands) - 1: 0},
        cost_estimate=estimate(4 * number * g.cap * length * 128),
        name="place",
    )(*operands)


def attend_kernel(g, chunks, page_len, width, local, *refs):
    owner, fill, query, old = refs[:4]
    blocks = refs[4:4 + len(chunks) * (g.groups - 1)]
    (out, stage, scores, seq_lane, seq_max, seq_total, seq_sum, sems) = refs[4 + len(blocks):]
    seqs, kj, _ = query.shape
    heads = g.rows // page_len
    group = kj // heads
    offset = pl.multiple_of(lax.axis_index("head") * g.rows, 8)
    copies = [pltpu.make_async_copy(
        old.at[:, pl.ds(offset, g.rows), :], stage.at[pl.ds(0, g.pages_own)], sems.at[0])]
    for j in range(1, g.groups):
        for c, (start, length) in enumerate(chunks):
            i = (j - 1) * len(chunks) + c
            copies.append(pltpu.make_async_copy(
                blocks[i], stage.at[pl.ds(j * g.pages_own, g.pages_own), pl.ds(start, length), :],
                sems.at[i + 1]))
    for copy in copies:
        copy.start()
    seq_lane[...] = jnp.full_like(seq_lane, NEG_FILL)
    seq_total[...] = jnp.zeros_like(seq_total)
    seq_sum[...] = jnp.zeros_like(seq_sum)
    for copy in copies:
        copy.wait()
    token = lax.broadcasted_iota(jnp.int32, (kj, page_len), 1)
    scale = width ** -0.5

    def page(p, k):
        return stage[p, k * page_len:(k + 1) * page_len, :]

    @pl.loop(0, g.page_count, unroll=8)
    def _(p):
        s = owner[p]
        query_rows = query[s]
        tiles = [lax.dot_general(
            query_rows[k * group:(k + 1) * group], page(p, k), (((1,), (1,)), ((), ())),
            preferred_element_type=jnp.float32) for k in range(heads)]
        tile = jnp.concatenate(tiles, 0) * scale
        tile = jnp.where(token < fill[p], tile, NEG_FILL)
        scores[p] = tile
        seq_lane[s] = jnp.maximum(seq_lane[s], tile)

    @pl.loop(0, seqs, unroll=4)
    def _(s):
        seq_max[s] = jnp.broadcast_to(
            jnp.max(seq_lane[s], axis=1, keepdims=True), (kj, page_len))

    @pl.loop(0, g.page_count, unroll=8)
    def _(p):
        s = owner[p]
        tile = scores[p]
        live = token < fill[p]
        weights = jnp.where(live, jnp.exp(tile - seq_max[s]), 0.0)
        high = weights.astype(jnp.bfloat16)
        low = (weights - high.astype(jnp.float32)).astype(jnp.bfloat16)
        sums = []
        for k in range(heads):
            here = slice(k * group, (k + 1) * group)
            both = jnp.dot(jnp.concatenate([high[here], low[here]], 0), page(p, k),
                           preferred_element_type=jnp.float32)
            sums.append(both[:group] + both[group:])
        seq_total[s] = seq_total[s] + weights
        seq_sum[s] = seq_sum[s] + jnp.concatenate(sums, 0)

    lane = lax.broadcasted_iota(jnp.int32, (kj, 128), 1)
    diagonal = lane == lax.broadcasted_iota(jnp.int32, (kj, 128), 0)
    shared = 128 // width

    @pl.loop(0, g.peers)
    def _(t):
        lines = []
        for i in range(local):
            s = t * local + i
            total = jnp.sum(seq_total[s], axis=1, keepdims=True)
            some = total > 0.0
            safe = jnp.where(some, total, 1.0)
            value = jnp.where(some, seq_sum[s] / safe, 0.0)
            if i % shared:
                value = pltpu.roll(value, 128 - width * (i % shared), 1)
                value = jnp.where(lane < 128 - width * (i % shared), value, tile)
            tile = value
            if i % shared == shared - 1 or i == local - 1:
                row = i // shared * kj
                out[t, row:row + kj, :] = tile.astype(jnp.bfloat16)
            log = jnp.where(some, seq_max[s, :, :1] + jnp.log(safe), NEG_FILL)
            log = jnp.broadcast_to(log, (kj, 128))
            for _ in range(3):
                part = log.astype(jnp.bfloat16).astype(jnp.float32)
                log = log - part
                lines.append(jnp.sum(jnp.where(diagonal, part, 0.0), axis=0, keepdims=True))
        while len(lines) % 8:
            lines.append(jnp.zeros((1, 128), jnp.float32))
        parts = (local + shared - 1) // shared * kj
        out[t, parts:parts + len(lines), :] = jnp.concatenate(lines, 0).astype(jnp.bfloat16)


def attend(g, owner, fill, query, old, received, chunks, width, page_len):
    seqs, kj, _ = query.shape
    local = seqs // g.peers
    extra = -(-local // (128 // width)) * kj + (3 * local + 7) // 8 * 8
    blocks = [received[c][j] for j in range(g.groups - 1) for c in range(len(chunks))]
    return pl.pallas_call(
        functools.partial(attend_kernel, g, chunks, page_len, width, local),
        out_shape=jax.ShapeDtypeStruct((g.peers, extra, 128), jnp.bfloat16),
        in_specs=[SMEM, SMEM, VMEM] + [HBM] * (1 + len(blocks)),
        out_specs=VMEM,
        scratch_shapes=[
            pltpu.VMEM((g.page_count, g.rows, 128), jnp.bfloat16),
            pltpu.VMEM((g.page_count, kj, page_len), jnp.float32),
            pltpu.VMEM((seqs, kj, page_len), jnp.float32),
            pltpu.VMEM((seqs, kj, page_len), jnp.float32),
            pltpu.VMEM((seqs, kj, page_len), jnp.float32),
            pltpu.VMEM((seqs, kj, 128), jnp.float32),
            pltpu.SemaphoreType.DMA((len(blocks) + 1,)),
        ],
        cost_estimate=pl.CostEstimate(
            flops=g.page_count * kj * page_len * 512 * 16,
            bytes_accessed=2 * g.page_count * g.rows * 128,
            transcendentals=g.page_count * kj * page_len),
        name="attend",
    )(owner, fill, query, old, *blocks)


def page_layout(dest, seq_pages, last_fill, page_len, page_count, peers):
    position = dest % page_count * peers + dest // page_count
    seqs = seq_pages.shape[0]
    ids = jnp.arange(seqs, dtype=jnp.int32)
    ends = jnp.sum(jnp.where(ids[:, None] <= ids[None, :], seq_pages[:, None], 0), axis=0)
    owner = jnp.sum((position[:, None] >= ends[None, :]).astype(jnp.int32), axis=1)
    member = owner[:, None] == ids[None, :]
    last = jnp.any(member & (position[:, None] == ends[None, :] - 1), axis=1)
    owner_fill = jnp.sum(jnp.where(member, last_fill[None, :], 0), axis=1)
    return owner, jnp.where(last, owner_fill, page_len)


def per_device(old_cache, page_dest, seq_pages, last_fill, queries):
    pages_own, all_heads, page_len, double = old_cache.shape
    groups, peers = lax.axis_size("head"), lax.axis_size("seq")
    head = lax.axis_index("head").astype(jnp.int32)
    width = double // 2
    heads = all_heads // groups
    rows = heads * page_len
    g = Geometry(pages_own, groups, peers, rows)
    seqs = queries.shape[0]
    kj = heads * (queries.shape[2] // width)
    edges = [0]
    for c in range(1, len(SHARES) + 1):
        edges.append(max(rows * sum(SHARES[:c]) // sum(SHARES) // 8 * 8, edges[-1] + 8))
    chunks = tuple((a, b - a) for a, b in zip(edges, edges[1:]))
    last = len(chunks) - 1
    old = old_cache.reshape(pages_own, all_heads * page_len, double)

    def swap(x, j):
        return lax.ppermute(x, "head", [(i, (i + j) % groups) for i in range(groups)])

    far, near = tuple(range(peers // 2, peers)), tuple(range(peers // 2))

    def route(blocks, ks):
        return [block if k == 0 else lax.ppermute(
            block, "seq", [(i, partner(i, k, peers)) for i in range(peers)])
            for k, block in zip(ks, blocks)]

    dests = [page_dest] + [swap(page_dest, j) for j in range(1, groups)]
    dest = jnp.concatenate(dests)
    received, source = [], old
    for start, length in chunks:
        pieces = []
        for j in range(1, groups):
            other = (head + j) % groups
            pieces.append(lax.dynamic_slice(
                source, (0, other * rows + start, 0), (pages_own, length, double)))
        source, pieces = lax.optimization_barrier((source, pieces))
        received.append([swap(piece, j) for j, piece in enumerate(pieces, 1)])
    query = jnp.pad(queries.reshape(seqs, kj, width), ((0, 0), (0, 0), (0, double - width)))
    owner, fill = page_layout(dest, seq_pages, last_fill, page_len, g.page_count, peers)
    pack_args = (dests, old)
    incoming, forwarded, tail = [], {}, None
    first_all = KINDS.index("all")
    pending = []
    for c, (kind, chunk) in enumerate(zip(KINDS, chunks)):
        if c == last:
            tail = attend(g, owner, fill, query, old, received, chunks, width, page_len)
        blocks = pack(g, None if kind == "all" else far, *pack_args, (chunk,),
                      received[c:c + 1], tail, c == first_all, kind != "far")
        if kind == "all":
            blocks = [lax.all_to_all(
                blocks[0], "seq", split_axis=0, concat_axis=0, tiled=True)]
            incoming.append((None, blocks, (chunk,), ()))
        elif kind == "far":
            incoming.append((far, route(blocks, far), (chunk,), ()))
        else:
            forwarded[c] = route(blocks, far[:1])[0]
        if kind != "all":
            pending.append(c)
        if pending and kind != "fwd":
            passed = tuple(i for i in pending if i in forwarded)
            blocks = pack(g, near, *pack_args, tuple(chunks[i] for i in pending),
                          [received[i] for i in pending], single=False,
                          passed=tuple(chunks[i][1] for i in passed),
                          forwarded=[forwarded[i] for i in passed])
            blocks = route(blocks, near)
            incoming.append((near, blocks, tuple(chunks[i] for i in pending),
                             tuple(chunks[i] for i in passed)))
            pending = []
    labels = read_labels(g, incoming[0][1][0], g.cap * chunks[first_all][1])
    cache = None
    for i, (ks, blocks, pieces, passed) in enumerate(incoming):
        merged = (seqs // peers, width, kj) if i == len(incoming) - 1 else None
        shape = (seqs // peers, heads, kj // heads * width)
        cache, *attended = place(
            g, ks, labels, blocks, cache, pieces, passed, merged, shape)
    return cache.reshape(g.page_count, heads, page_len, double), attended[0]


def solution(mesh):
    in_specs = (
        P(("seq", "head"), None, None, None),
        P(("seq", "head")),
        P(),
        P(),
        P(None, "head", None),
    )
    out_specs = (P("seq", "head", None, None), P("seq", "head", None))
    return jax.shard_map(
        per_device, mesh=mesh, in_specs=in_specs, out_specs=out_specs, check_vma=False
    )
```

```python
import functools
import jax
import jax.numpy as jnp
from jax import lax
from jax.experimental import pallas as pl
from jax.experimental.pallas import tpu as pltpu
from jax.sharding import PartitionSpec as P

NEG_FILL = -1e30
LABEL_ROWS = 8
SHARES = (1, 2, 3, 4, 8, 9, 5)
KINDS = ("fwd", "fwd", "fwd", "fwd", "all", "far", "all")

HBM = pl.BlockSpec(memory_space=pltpu.HBM)
SMEM = pl.BlockSpec(memory_space=pltpu.SMEM)
VMEM = pl.BlockSpec(memory_space=pltpu.VMEM)


def partner(me, k, peers):
    if peers & (peers - 1) == 0:
        return me ^ k
    return (me + k) % peers


def sender(me, k, peers):
    if peers & (peers - 1) == 0:
        return me ^ k
    return (me + peers - k) % peers


class Geometry:
    def __init__(self, pages_own, groups, peers, rows):
        self.pages_own, self.groups, self.peers, self.rows = pages_own, groups, peers, rows
        self.page_count = pages_own * groups
        self.cap = self.page_count // min(peers, 16)
        self.full = peers * self.cap == self.page_count


def spread(pieces):
    offset, laid = 0, []
    for start, length in pieces:
        laid.append((start, length, offset))
        offset += length
    return laid, offset


def granted(*sizes):
    return pltpu.CompilerParams(vmem_limit_bytes=(4 << 20) + sum(sizes))


def estimate(moved):
    return pl.CostEstimate(flops=moved * 4, bytes_accessed=moved, transcendentals=0)


def pack_kernel(g, ks, single, pieces, passed, extra, label, *refs):
    laid, length = spread(pieces)
    dests, old, refs = refs[:g.groups], refs[g.groups], refs[g.groups + 1:]
    count = len(pieces) * (g.groups - 1)
    received, refs = refs[:count], refs[count:]
    head, me = lax.axis_index("head"), lax.axis_index("seq")
    forwarded, refs = refs[:len(passed)], refs[len(passed):]
    tail = None
    if extra and not label:
        tail, refs = refs[0], refs[1:]
    number = g.peers if ks is None else len(ks)
    if single:
        outs, refs = [refs[0].at[i] for i in range(number)], refs[1:]
    else:
        outs, refs = refs[:number], refs[number:]
    if ks is None:
        targets = list(range(g.peers))
    else:
        targets = [partner(me, k, g.peers) for k in ks]
    stage, counts, order, slot, in_sem, out_sem = refs[:6]
    pass_stages, refs = refs[6:6 + len(passed)], refs[6 + len(passed):]
    copies = []
    for c, (start, size, offset) in enumerate(laid):
        row = pl.multiple_of(head * g.rows + start, 8)
        copies.append(pltpu.make_async_copy(
            old.at[:, pl.ds(row, size), :],
            stage.at[pl.ds(0, g.pages_own), pl.ds(offset, size), :], in_sem.at[c]))
        for j in range(1, g.groups):
            i = (j - 1) * len(pieces) + c
            copies.append(pltpu.make_async_copy(
                received[i],
                stage.at[pl.ds(j * g.pages_own, g.pages_own), pl.ds(offset, size), :],
                in_sem.at[len(pieces) + i]))
    arrivals = []
    if passed:
        pass_in, pass_out = refs
        arrivals = [pltpu.make_async_copy(block, place, pass_in.at[c]) for c, (block, place)
                    in enumerate(zip(forwarded, pass_stages))]
    for copy in copies + arrivals:
        copy.start()

    @pl.loop(0, g.peers, unroll=8)
    def _(t):
        counts[t] = 0

    if not g.full:
        @pl.loop(0, g.peers * g.cap)
        def _(i):
            order[i] = -1

    for j, dest in enumerate(dests):
        @pl.loop(0, g.pages_own, unroll=8)
        def _(i):
            d = dest[i]
            if g.page_count & (g.page_count - 1) == 0:
                t = lax.shift_right_logical(d, g.page_count.bit_length() - 1)
            else:
                t = d // g.page_count
            n = counts[t]
            counts[t] = n + 1
            order[t * g.cap + n] = j * g.pages_own + i
            if label:
                slot[t * g.cap + n] = d - t * g.page_count

    for i, t in enumerate(targets):
        block = outs[i]
        if tail is not None:
            block[g.cap * length:g.cap * length + extra // 2, :] = tail[t]
            block[g.cap * length + extra // 2:, :] = tail[partner(t, g.peers // 2, g.peers)]
        if label:
            lane = lax.broadcasted_iota(jnp.int32, (extra, 128), 1)
            tile = jnp.full((extra, 128), -1, jnp.int32)
            for n in range(g.cap):
                value = slot[t * g.cap + n]
                if not g.full:
                    value = jnp.where(order[t * g.cap + n] >= 0, value, -1)
                tile = jnp.where(lane == n, value, tile)
            block[g.cap * length:, :] = tile.astype(jnp.float32).astype(jnp.bfloat16)
    for copy in copies:
        copy.wait()
    if not passed:
        for i, t in enumerate(targets):
            for n in range(g.cap):
                p = order[t * g.cap + n]
                outs[i][n * length:(n + 1) * length, :] = stage[p if g.full else jnp.maximum(p, 0)]
        return

    def page_copy(i, n, p):
        return pltpu.make_async_copy(
            stage.at[p], outs[i].at[pl.ds(n * length, length), :], out_sem.at[i])

    for step in ("start",) if g.full else ("start", "wait"):
        for i, t in enumerate(targets):
            for n in range(g.cap):
                p = order[t * g.cap + n]
                if g.full:
                    page_copy(i, n, p).start()
                else:
                    @pl.when(p >= 0)
                    def _():
                        getattr(page_copy(i, n, p), step)()
    base, passes = g.cap * length, []
    for c, size in enumerate(passed):
        arrivals[c].wait()
        for i in range(number):
            passes.append(pltpu.make_async_copy(
                pass_stages[c].at[i], outs[i].at[pl.ds(base, g.cap * size), :], pass_out.at[c, i]))
            passes[-1].start()
        base += g.cap * size
    if g.full:
        for i in range(len(targets)):
            block = outs[i].at[pl.ds(0, g.cap * length), :]
            pltpu.make_async_copy(block, block, out_sem.at[i]).wait()
    for copy in passes:
        copy.wait()


def pack(g, ks, dests, old, pieces, received, tail=None, label=False, single=True,
         passed=(), forwarded=()):
    _, length = spread(pieces)
    extra = LABEL_ROWS if label else (2 * tail.shape[1] if tail is not None else 0)
    blocks = [received[c][j] for j in range(g.groups - 1) for c in range(len(pieces))]
    operands = [*dests, old, *blocks, *forwarded] + ([tail] if tail is not None else [])
    shape = (g.cap * (length + sum(passed)) + extra, 128)
    number = g.peers if ks is None else len(ks)
    if single:
        outs = [jax.ShapeDtypeStruct((number,) + shape, jnp.bfloat16)]
    else:
        outs = [jax.ShapeDtypeStruct(shape, jnp.bfloat16)] * number
    scratch = [
        pltpu.VMEM((g.page_count, length, 128), jnp.bfloat16),
        pltpu.SMEM((g.peers,), jnp.int32),
        pltpu.SMEM((g.peers * g.cap,), jnp.int32),
        pltpu.SMEM((g.peers * g.cap,), jnp.int32),
        pltpu.SemaphoreType.DMA((len(pieces) * g.groups,)),
        pltpu.SemaphoreType.DMA((number,)),
    ]
    scratch += [pltpu.VMEM((number, g.cap * size, 128), jnp.bfloat16) for size in passed]
    if passed:
        scratch += [pltpu.SemaphoreType.DMA((len(passed),)),
                    pltpu.SemaphoreType.DMA((len(passed), number))]
    return pl.pallas_call(
        functools.partial(pack_kernel, g, ks, single, pieces, passed, extra, label),
        out_shape=outs,
        in_specs=[SMEM] * g.groups + [HBM] * (1 + len(blocks) + len(forwarded))
        + ([VMEM] if tail is not None else []),
        out_specs=[HBM if passed else VMEM] * len(outs),
        scratch_shapes=scratch,
        cost_estimate=estimate(4 * number * g.cap * length * 128),
        name="pack",
    )(*operands)


def labels_kernel(g, row, blocks, out, raw, lines, sem, out_sem):
    copy = pltpu.make_async_copy(blocks.at[:, pl.ds(row, LABEL_ROWS), :], raw, sem)
    copy.start()
    copy.wait()
    for i in range(g.peers):
        lines[i:i + 1, :] = raw[i].astype(jnp.float32)[:1].astype(jnp.int32)
    move = pltpu.make_async_copy(lines, out, out_sem)
    move.start()
    move.wait()


def read_labels(g, blocks, row):
    return pl.pallas_call(
        functools.partial(labels_kernel, g, row),
        out_shape=jax.ShapeDtypeStruct((g.peers, 128), jnp.int32),
        in_specs=[HBM],
        out_specs=SMEM,
        scratch_shapes=[
            pltpu.VMEM((g.peers, LABEL_ROWS, 128), jnp.bfloat16),
            pltpu.VMEM((g.peers, 128), jnp.int32),
            pltpu.SemaphoreType.DMA,
            pltpu.SemaphoreType.DMA,
        ],
        compiler_params=granted(),
        cost_estimate=estimate(g.peers * 4096),
        name="labels",
    )(blocks)


def entry_rows(local, kj):
    return local * kj + (3 * local + 7) // 8 * 8


def write_entries(out, entries, width):
    kj = entries[0][0].shape[0]
    lane = lax.broadcasted_iota(jnp.int32, (kj, 128), 1)
    diagonal = lane == lax.broadcasted_iota(jnp.int32, (kj, 128), 0)
    lines = []
    for i, (value, log) in enumerate(entries):
        high = value.astype(jnp.bfloat16).astype(jnp.float32)
        low = pltpu.roll(value - high, 128 - width, 1)
        out[i * kj:(i + 1) * kj, :] = jnp.where(lane < width, low, high).astype(jnp.bfloat16)
        for _ in range(3):
            part = log.astype(jnp.bfloat16).astype(jnp.float32)
            log = log - part
            lines.append(jnp.sum(jnp.where(diagonal, part, 0.0), axis=0, keepdims=True))
    while len(lines) % 8:
        lines.append(jnp.zeros((1, 128), jnp.float32))
    row = len(entries) * kj
    out[row:row + len(lines), :] = jnp.concatenate(lines, 0).astype(jnp.bfloat16)


def merge_entries(tails, local, width, kj):
    lane = lax.broadcasted_iota(jnp.int32, (kj, 128), 1)
    diagonal = lane == lax.broadcasted_iota(jnp.int32, (kj, 128), 0)

    def column(line):
        spread_line = jnp.where(diagonal, jnp.broadcast_to(line, (kj, 128)), 0.0)
        return jnp.broadcast_to(jnp.sum(spread_line, axis=1, keepdims=True), (kj, 128))

    lines = [tail[local * kj:, :].astype(jnp.float32) for tail in tails]
    merged = []
    for s in range(local):
        logs = [jnp.sum(line[3 * s:3 * s + 3], axis=0, keepdims=True) for line in lines]
        top = functools.reduce(jnp.maximum, logs)
        scales = [jnp.exp(log - top) for log in logs]
        total = sum(scales)
        summed = jnp.zeros((kj, 128), jnp.float32)
        for tail, scale in zip(tails, scales):
            summed = summed + column(scale / total) * tail[s * kj:(s + 1) * kj, :].astype(jnp.float32)
        merged.append((summed + pltpu.roll(summed, width, 1), column(top + jnp.log(total))))
    return merged


def reduce_kernel(row, local, width, kj, *refs):
    blocks, (mine, across, tail, sems) = refs[:-4], refs[-4:]
    extra = entry_rows(local, kj)
    copies = [pltpu.make_async_copy(block.at[pl.ds(row, 2 * extra), :], tail.at[i], sems.at[i])
              for i, block in enumerate(blocks)]
    for copy in copies:
        copy.start()
    for copy in copies:
        copy.wait()
    for out, first in ((mine, 0), (across, extra)):
        tails = [tail[i, first:first + extra, :] for i in range(len(blocks))]
        write_entries(out, merge_entries(tails, local, width, kj), width)


def reduce_near(blocks, row, local, width, kj):
    extra = entry_rows(local, kj)
    return pl.pallas_call(
        functools.partial(reduce_kernel, row, local, width, kj),
        out_shape=[jax.ShapeDtypeStruct((extra, 128), jnp.bfloat16)] * 2,
        in_specs=[HBM] * len(blocks),
        out_specs=[VMEM] * 2,
        scratch_shapes=[
            pltpu.VMEM((len(blocks), 2 * extra, 128), jnp.bfloat16),
            pltpu.SemaphoreType.DMA((len(blocks),)),
        ],
        compiler_params=granted(2 * len(blocks) * 2 * extra * 128),
        cost_estimate=estimate(len(blocks) * extra * 2048),
        name="reduce",
    )(*blocks)


def place_kernel(g, ks, pieces, passed, first, merged, *refs):
    laid, length = spread(pieces)
    labels, refs = refs[0], refs[1:]
    me = lax.axis_index("seq")
    if ks is None:
        blocks, refs = [refs[0].at[t] for t in range(g.peers)], refs[1:]
        indices = list(range(g.peers))
    else:
        blocks, refs = refs[:len(ks)], refs[len(ks):]
        indices = [sender(me, k, g.peers) for k in ks]
    if merged:
        tails, refs = refs[:2], refs[2:]
    refs = refs if first else refs[1:]
    cache, refs = refs[0], refs[1:]
    if merged:
        attended, refs = refs[0], refs[1:]
    out_sem = refs[0]

    def each_page(act):
        for i, (block, index) in enumerate(zip(blocks, indices)):
            for n in range(g.cap):
                label = labels[index, n]

                def run():
                    for start, size, offset in laid:
                        getattr(pltpu.make_async_copy(
                            block.at[pl.ds(n * length + offset, size), :],
                            cache.at[label, pl.ds(start, size), :], out_sem.at[i]), act)()

                if g.full:
                    run()
                else:
                    pl.when(label >= 0)(run)
                if not passed:
                    continue
                other = labels[sender(index, g.peers // 2, g.peers), n]

                def run_passed():
                    base = g.cap * length
                    for start, size in passed:
                        getattr(pltpu.make_async_copy(
                            block.at[pl.ds(base + n * size, size), :],
                            cache.at[other, pl.ds(start, size), :], out_sem.at[i]), act)()
                        base += g.cap * size

                if g.full:
                    run_passed()
                else:
                    pl.when(other >= 0)(run_passed)

    each_page("start")
    if merged:
        local, width, kj = merged
        group = attended.shape[2] // width
        for i, (value, _) in enumerate(merge_entries(tails, local, width, kj)):
            value = value[:, 128 - width:].astype(jnp.bfloat16)
            for row in range(kj):
                k, j = row // group, row % group
                attended[i, k:k + 1, j * width:(j + 1) * width] = value[row:row + 1]
    if g.full:
        for i, block in enumerate(blocks):
            rows = g.cap * (length + sum(size for _, size in passed))
            moved = block.at[pl.ds(0, rows), :]
            pltpu.make_async_copy(moved, moved, out_sem.at[i]).wait()
    else:
        each_page("wait")


def place(g, ks, labels, blocks, cache, pieces, passed=(), merged=None, shape=None, tails=()):
    first = cache is None
    _, length = spread(pieces)
    operands = [labels, *blocks, *tails] + ([] if first else [cache])
    outs = [jax.ShapeDtypeStruct((g.page_count, g.rows, 128), jnp.bfloat16)]
    out_specs = [HBM]
    if merged:
        outs.append(jax.ShapeDtypeStruct(shape, jnp.bfloat16))
        out_specs.append(VMEM)
    number = g.peers if ks is None else len(ks)
    return pl.pallas_call(
        functools.partial(place_kernel, g, ks, pieces, passed, first, merged),
        out_shape=outs,
        in_specs=[SMEM] + [VMEM] * (len(blocks) + len(tails)) + [HBM] * (0 if first else 1),
        out_specs=out_specs,
        scratch_shapes=[pltpu.SemaphoreType.DMA((number,))],
        compiler_params=granted(2 * number * blocks[0].shape[-2] * 128),
        input_output_aliases={} if first else {len(operands) - 1: 0},
        cost_estimate=estimate(4 * number * g.cap * length * 128),
        name="place",
    )(*operands)


def attend_kernel(g, chunks, page_len, width, local, *refs):
    owner, fill, query, old = refs[:4]
    blocks = refs[4:4 + len(chunks) * (g.groups - 1)]
    (out, stage, scores, seq_lane, seq_max, seq_total, seq_sum, sems) = refs[4 + len(blocks):]
    seqs, kj, _ = query.shape
    heads = g.rows // page_len
    group = kj // heads
    offset = pl.multiple_of(lax.axis_index("head") * g.rows, 8)
    copies = [pltpu.make_async_copy(
        old.at[:, pl.ds(offset, g.rows), :], stage.at[pl.ds(0, g.pages_own)], sems.at[0])]
    for j in range(1, g.groups):
        for c, (start, length) in enumerate(chunks):
            i = (j - 1) * len(chunks) + c
            copies.append(pltpu.make_async_copy(
                blocks[i], stage.at[pl.ds(j * g.pages_own, g.pages_own), pl.ds(start, length), :],
                sems.at[i + 1]))
    for copy in copies:
        copy.start()
    seq_lane[...] = jnp.full_like(seq_lane, NEG_FILL)
    seq_total[...] = jnp.zeros_like(seq_total)
    seq_sum[...] = jnp.zeros_like(seq_sum)
    for copy in copies:
        copy.wait()
    token = lax.broadcasted_iota(jnp.int32, (kj, page_len), 1)
    scale = width ** -0.5

    def page(p, k):
        return stage[p, k * page_len:(k + 1) * page_len, :]

    @pl.loop(0, g.page_count, unroll=8)
    def _(p):
        s = owner[p]
        query_rows = query[s]
        tiles = [lax.dot_general(
            query_rows[k * group:(k + 1) * group], page(p, k), (((1,), (1,)), ((), ())),
            preferred_element_type=jnp.float32) for k in range(heads)]
        tile = jnp.concatenate(tiles, 0) * scale
        tile = jnp.where(token < fill[p], tile, NEG_FILL)
        scores[p] = tile
        seq_lane[s] = jnp.maximum(seq_lane[s], tile)

    @pl.loop(0, seqs, unroll=4)
    def _(s):
        seq_max[s] = jnp.broadcast_to(
            jnp.max(seq_lane[s], axis=1, keepdims=True), (kj, page_len))

    @pl.loop(0, g.page_count, unroll=8)
    def _(p):
        s = owner[p]
        tile = scores[p]
        live = token < fill[p]
        weights = jnp.where(live, jnp.exp(tile - seq_max[s]), 0.0)
        high = weights.astype(jnp.bfloat16)
        low = (weights - high.astype(jnp.float32)).astype(jnp.bfloat16)
        sums = []
        for k in range(heads):
            here = slice(k * group, (k + 1) * group)
            both = jnp.dot(jnp.concatenate([high[here], low[here]], 0), page(p, k),
                           preferred_element_type=jnp.float32)
            sums.append(both[:group] + both[group:])
        seq_total[s] = seq_total[s] + weights
        seq_sum[s] = seq_sum[s] + jnp.concatenate(sums, 0)

    @pl.loop(0, g.peers, unroll=4)
    def _(t):
        entries = []
        for i in range(local):
            s = t * local + i
            total = jnp.sum(seq_total[s], axis=1, keepdims=True)
            some = total > 0.0
            safe = jnp.where(some, total, 1.0)
            value = jnp.where(some, seq_sum[s] / safe, 0.0)
            log = jnp.where(some, seq_max[s, :, :1] + jnp.log(safe), NEG_FILL)
            entries.append((value, jnp.broadcast_to(log, (kj, 128))))
        write_entries(out.at[t], entries, width)


def attend(g, owner, fill, query, old, received, chunks, width, page_len):
    seqs, kj, _ = query.shape
    local = seqs // g.peers
    extra = entry_rows(local, kj)
    blocks = [received[c][j] for j in range(g.groups - 1) for c in range(len(chunks))]
    return pl.pallas_call(
        functools.partial(attend_kernel, g, chunks, page_len, width, local),
        out_shape=jax.ShapeDtypeStruct((g.peers, extra, 128), jnp.bfloat16),
        in_specs=[SMEM, SMEM, VMEM] + [HBM] * (1 + len(blocks)),
        out_specs=VMEM,
        scratch_shapes=[
            pltpu.VMEM((g.page_count, g.rows, 128), jnp.bfloat16),
            pltpu.VMEM((g.page_count, kj, page_len), jnp.float32),
            pltpu.VMEM((seqs, kj, page_len), jnp.float32),
            pltpu.VMEM((seqs, kj, page_len), jnp.float32),
            pltpu.VMEM((seqs, kj, page_len), jnp.float32),
            pltpu.VMEM((seqs, kj, 128), jnp.float32),
            pltpu.SemaphoreType.DMA((len(blocks) + 1,)),
        ],
        cost_estimate=pl.CostEstimate(
            flops=g.page_count * kj * page_len * 512 * 16,
            bytes_accessed=2 * g.page_count * g.rows * 128,
            transcendentals=g.page_count * kj * page_len),
        name="attend",
    )(owner, fill, query, old, *blocks)


def page_layout(dest, seq_pages, last_fill, page_len, page_count, peers):
    position = dest % page_count * peers + dest // page_count
    seqs = seq_pages.shape[0]
    ids = jnp.arange(seqs, dtype=jnp.int32)
    ends = jnp.sum(jnp.where(ids[:, None] <= ids[None, :], seq_pages[:, None], 0), axis=0)
    owner = jnp.sum((position[:, None] >= ends[None, :]).astype(jnp.int32), axis=1)
    member = owner[:, None] == ids[None, :]
    last = jnp.any(member & (position[:, None] == ends[None, :] - 1), axis=1)
    owner_fill = jnp.sum(jnp.where(member, last_fill[None, :], 0), axis=1)
    return owner, jnp.where(last, owner_fill, page_len)


def per_device(old_cache, page_dest, seq_pages, last_fill, queries):
    pages_own, all_heads, page_len, double = old_cache.shape
    groups, peers = lax.axis_size("head"), lax.axis_size("seq")
    head = lax.axis_index("head").astype(jnp.int32)
    width = double // 2
    heads = all_heads // groups
    rows = heads * page_len
    g = Geometry(pages_own, groups, peers, rows)
    seqs = queries.shape[0]
    kj = heads * (queries.shape[2] // width)
    edges = [0]
    for c in range(1, len(SHARES) + 1):
        edges.append(max(rows * sum(SHARES[:c]) // sum(SHARES) // 8 * 8, edges[-1] + 8))
    chunks = tuple((a, b - a) for a, b in zip(edges, edges[1:]))
    old = old_cache.reshape(pages_own, all_heads * page_len, double)

    def swap(x, j):
        return lax.ppermute(x, "head", [(i, (i + j) % groups) for i in range(groups)])

    far, near = tuple(range(peers // 2, peers)), tuple(range(peers // 2))

    def route(blocks, ks):
        return [block if k == 0 else lax.ppermute(
            block, "seq", [(i, partner(i, k, peers)) for i in range(peers)])
            for k, block in zip(ks, blocks)]

    dests = [page_dest] + [swap(page_dest, j) for j in range(1, groups)]
    dest = jnp.concatenate(dests)
    received, source = [], old
    for start, length in chunks:
        pieces = []
        for j in range(1, groups):
            other = (head + j) % groups
            pieces.append(lax.dynamic_slice(
                source, (0, other * rows + start, 0), (pages_own, length, double)))
        source, pieces = lax.optimization_barrier((source, pieces))
        received.append([swap(piece, j) for j, piece in enumerate(pieces, 1)])
    query = jnp.pad(queries.reshape(seqs, kj, width), ((0, 0), (0, 0), (0, double - width)))
    owner, fill = page_layout(dest, seq_pages, last_fill, page_len, g.page_count, peers)
    pack_args = (dests, old)
    incoming, forwarded, tail = [], {}, None
    first_all = KINDS.index("all")
    pending = []
    for c, (kind, chunk) in enumerate(zip(KINDS, chunks)):
        blocks = pack(g, None if kind == "all" else far, *pack_args, (chunk,),
                      received[c:c + 1], None, c == first_all, kind != "far")
        if kind == "all":
            blocks = [lax.all_to_all(
                blocks[0], "seq", split_axis=0, concat_axis=0, tiled=True)]
            incoming.append((None, blocks, (chunk,), ()))
        elif kind == "far":
            incoming.append((far, route(blocks, far), (chunk,), ()))
        else:
            forwarded[c] = route(blocks, far[:1])[0]
        if kind != "all":
            pending.append(c)
        if pending and kind != "fwd":
            if kind == "far":
                tail = attend(
                    g, owner, fill, query, old, received, chunks, width, page_len)
            passed = tuple(i for i in pending if i in forwarded)
            blocks = pack(g, near, *pack_args, tuple(chunks[i] for i in pending),
                          [received[i] for i in pending], tail, single=False,
                          passed=tuple(chunks[i][1] for i in passed),
                          forwarded=[forwarded[i] for i in passed])
            blocks = route(blocks, near)
            incoming.append((near, blocks, tuple(chunks[i] for i in pending),
                             tuple(chunks[i] for i in passed)))
            if tail is not None:
                near_tails = (blocks, g.cap * sum(chunks[i][1] for i in pending))
            pending = []
    labels = read_labels(g, incoming[0][1][0], g.cap * chunks[first_all][1])
    mine, across = reduce_near(*near_tails, seqs // peers, width, kj)
    tails = [mine] + route([across], far[:1])
    cache = None
    for i, (ks, blocks, pieces, passed) in enumerate(incoming):
        merged = (seqs // peers, width, kj) if i == len(incoming) - 1 else None
        shape = (seqs // peers, heads, kj // heads * width)
        cache, *attended = place(
            g, ks, labels, blocks, cache, pieces, passed, merged, shape,
            tails if merged else ())
    return cache.reshape(g.page_count, heads, page_len, double), attended[0]


def solution(mesh):
    in_specs = (
        P(("seq", "head"), None, None, None),
        P(("seq", "head")),
        P(),
        P(),
        P(None, "head", None),
    )
    out_specs = (P("seq", "head", None, None), P("seq", "head", None))
    return jax.shard_map(
        per_device, mesh=mesh, in_specs=in_specs, out_specs=out_specs, check_vma=False
    )
```
